32 devices in a mesh: row: 8 (over y, x, core), col: 4 (over z).
Axes of the slice: x: 2, y: 2, z: 4, core: 2. Of those that a mesh axis runs over, the one named last changes fastest.
Arguments:
- acts: bfloat16 [512, 16384], P('row', 'col'), may hold values from -6 to 6
- grads: float32 [16384, 512], P('col', 'row'), may hold values from -24 to 24
Outputs:
- factor: float32 [16384, 16384], P('row', 'col')
- applied: float32 [16384, 512], P('row', 'col')
- solution: float32 [16384, 512], P('col', 'row')
The draws below stay inside these ranges and needn't reach their ends.
All inputs are finite; a program needn't handle non-finite values.
Results may differ from the reference program's by a relative error of at most 0.0003.
Values may be sent and summed in bfloat16 or wider, within the bound.
No kernel may reach another device: no remote copies, remote signals or barrier semaphores. Data moves between devices by JAX's collectives and lax.ppermute only.
A program may use at most 128 MiB of HBM per device.

```python
import math
import jax
import jax.numpy as jnp
from jax import lax

D = 16384
NRHS = 512
TOKENS = 512


def steps_of(own_key, extent, pieces, least, largest):
    factor_of, own = 1.0, jax.random.fold_in(own_key, 6)
    for dim, blocks in pieces:
        draws = jnp.exp(jax.random.uniform(jax.random.fold_in(own, dim), (blocks,), jnp.float32, least / len(pieces), largest / len(pieces)))
        factor_of = factor_of * jnp.repeat(draws, extent[dim] // blocks).reshape([-1 if axis == dim else 1 for axis in range(len(extent))])
    return factor_of


def scatter_about(own_key, extent, scale, bound, shards=(), held_as=jnp.bfloat16):
    factor_of = steps_of(own_key, extent, shards, -0.22, 0.18) if shards else 1.0
    entries = jax.random.normal(own_key, extent, jnp.float32) * scale * factor_of
    return jnp.minimum(jnp.maximum(entries, -bound), bound).astype(held_as)


def setup_inputs(seed: int = 0) -> dict:
    key_of = jax.random.split(jax.random.key(seed), 3)
    acts = scatter_about(key_of[0], (TOKENS, D), 1.0, 6.0, ((0, 8), (1, 4)))
    grads = scatter_about(key_of[1], (D, NRHS), 4.0, 24.0, ((0, 4), (1, 8)), jnp.float32)
    return dict(acts=acts, grads=grads)


damping = 1.0

def step_size(feature_count, token_count):
    return 1.0 / (damping + (1.0 + math.sqrt(feature_count / token_count)) ** 2)

def reference(acts, grads):
    token_count = acts.shape[0]
    omega_step = step_size(acts.shape[1], token_count)
    widened = acts.astype(jnp.float32)
    factor = jnp.dot(widened.T, widened, precision=lax.Precision.HIGHEST) / token_count
    applied = jnp.dot(factor, grads, precision=lax.Precision.HIGHEST) + damping * grads
    second = jnp.dot(factor, applied, precision=lax.Precision.HIGHEST) + damping * applied
    solution = 3.0 * omega_step * grads - 3.0 * omega_step ** 2 * applied + omega_step ** 3 * second
    return (factor, applied, solution)
```

```python
import math

import jax
import jax.numpy as jnp
from jax import lax
from jax.sharding import PartitionSpec as P


damping = 1.0


def step_size(feature_count, token_count):
    return 1.0 / (damping + (1.0 + math.sqrt(feature_count / token_count)) ** 2)


def split(value, axis):
    high = lax.reduce_precision(value, 8, 7)
    low = value - high
    return jnp.concatenate([high.astype(jnp.bfloat16), low.astype(jnp.bfloat16)], axis)


def merge(value):
    half = value.shape[0] // 2
    return value[:half] + value[half:]


def times(left, right, left_dim, right_dim):
    return lax.dot_general(
        left, right, (((left_dim,), (right_dim,)), ((), ())), preferred_element_type=jnp.float32
    )


def middle(z):
    return z in (1, 2)


def plan_inner(layers):
    if layers != 4:
        return [
            {(k, z): (z, k ^ turn) for k in range(layers) for z in range(layers)}
            for turn in range(layers)
        ], []
    flat = [
        {
            (k, z): (k ^ mask, z)
            for k in range(4)
            for z in range(4)
            if middle(z) or k ^ mask in (z, z ^ 1)
        }
        for mask in (1, 2, 3)
    ]
    outer = [
        {
            (k, z): ((2 if z == 1 else 0) + (turn ^ k), 0 if z == 1 else 3)
            for k in range(4)
            for z in (1, 2)
            if turn ^ k in (0, 1)
        }
        for turn in range(4)
    ]
    return flat, outer


def step(acts, grads):
    layers = lax.axis_size("col")
    lanes = lax.axis_size("row") // layers
    row_index = lax.axis_index("row")
    layer = lax.axis_index("col")
    group = row_index // lanes
    lane = row_index % lanes
    tokens, width = acts.shape
    share = width // lanes
    group_tokens = tokens * lanes
    token_count = group_tokens * layers
    omega = step_size(width * layers, token_count)
    bits = [1 << b for b in range(layers.bit_length() - 1)]

    def send(value, rule):
        pairs = []
        for k in range(layers):
            for j in range(lanes):
                for z in range(layers):
                    target = rule(k, j, z)
                    if target is not None:
                        to_k, to_j, to_z = target
                        pairs.append(
                            ((k * lanes + j) * layers + z, (to_k * lanes + to_j) * layers + to_z)
                        )
        return lax.ppermute(value, ("row", "col"), pairs)

    def shift(value, step):
        return send(value, lambda k, j, z: (k, (j + step) % lanes, z))

    def follow(value, plan):
        def rule(k, j, z):
            if (k, z) not in plan:
                return None
            to_k, to_z = plan[k, z]
            return (to_k, j, to_z)

        return send(value, rule)

    def put(whole, part, *spot):
        spot = spot + (0,) * (whole.ndim - len(spot))
        return lax.dynamic_update_slice(whole, part[(None,) * (whole.ndim - part.ndim)], spot)

    grads_t = grads.T

    panel = jnp.broadcast_to(acts, (layers, lanes, tokens, width))
    pieces = {0: acts}
    for mask in range(1, layers):
        pieces[mask] = send(acts, lambda k, j, z: (k ^ mask, j, z))
    swapped = [acts]
    for mask, piece in pieces.items():
        panel = put(panel, piece, group ^ mask, lane)
        for step in range(1, lanes):
            other = shift(piece, step)
            if mask == 0:
                swapped.append(other)
            panel = put(panel, other, group ^ mask, (lane - step) % lanes)
    panel = panel.reshape(token_count, width)

    mine = jnp.broadcast_to(
        lax.dynamic_slice_in_dim(acts, lane * share, share, 1), (lanes, tokens, share)
    )
    for step in range(1, lanes):
        cut = lax.dynamic_slice_in_dim(swapped[step], lane * share, share, 1)
        mine = put(mine, cut, (lane - step) % lanes)
    mine = put(mine, lax.dynamic_slice_in_dim(acts, lane * share, share, 1), lane)
    mine_t = mine.reshape(group_tokens, share).T

    flat, outer = plan_inner(layers)
    if layers == 4:
        held = jnp.broadcast_to(mine_t, (layers, share, group_tokens))
        ways = [
            ({0: 2, 3: 1}, (layer + 2) % 4),
            ({1: 2, 2: 1}, 3 - layer),
            ({0: 1, 1: 0, 2: 3, 3: 2}, layer ^ 1),
        ]
        for goes, spot in ways:
            part = send(mine_t, lambda k, j, z: (k, j, goes[z]) if z in goes else None)
            held = put(held, part, spot)
        held = put(held, mine_t, layer)

        def pick(index):
            return lax.dynamic_index_in_dim(held, index, 0, keepdims=False)

        inner_t = jnp.broadcast_to(pick(group), held.shape)
        for mask, plan in enumerate(flat, 1):
            inner_t = put(inner_t, follow(pick(group ^ mask), plan), group ^ mask)
        first = jnp.where(layer == 1, 2, 0)
        turned = [
            follow(pick(first + ((turn ^ group) & 1)), plan)
            for turn, plan in enumerate(outer)
        ]
        is_outer = ((layer == 0) & (group >= 2)) | ((layer == 3) & (group < 2))
        odd = group % 2 == 1
        inner_t = jnp.concatenate(
            [
                jnp.where(is_outer, jnp.where(odd, turned[p ^ 1], turned[p]), inner_t[p])
                for p in range(4)
            ],
            1,
        )
    else:
        inner_t = jnp.broadcast_to(mine_t, (layers, share, group_tokens))
        for turn, plan in enumerate(flat):
            inner_t = put(inner_t, follow(mine_t, plan), layer ^ turn)
        inner_t = inner_t.transpose(1, 0, 2).reshape(share, token_count)

    moved = []
    for step in range(lanes):
        part = lax.dynamic_slice_in_dim(grads_t, (lane + step) % lanes * share, share, 1)
        if step == 0:
            moved.append(send(part, lambda k, j, z: (z, j, k)))
        else:
            flip = layers // 2
            part = send(part, lambda k, j, z: (k ^ flip, (j + step) % lanes, z))
            moved.append(send(part, lambda k, j, z: (z, j, k ^ flip)))

    def layer_sum(value):
        for bit in bits:
            value = value + send(value, lambda k, j, z: (k, j, z ^ bit))
        return value

    def to_tokens(value):
        return merge(times(value, panel, 1, 1))

    def to_features(value):
        return merge(times(split(value * (1.0 / token_count), 0), panel, 1, 0))

    grads_split = split(grads_t, 0)
    u = to_tokens(grads_split)
    u = layer_sum(u)
    y = to_features(u) + damping * grads_t
    w = layer_sum(to_tokens(split(y, 0)))
    second = to_features(w) + damping * y
    solution_t = 3.0 * omega * grads_t - 3.0 * omega**2 * y + omega**3 * second

    u_near = jnp.where(group == layer, u, 0.0)
    for mask in range(1, layers):
        u_near = u_near + send(u, lambda k, j, z: (k ^ mask, j, z) if k == z else None)
    u_all = put(jnp.zeros((lanes,) + u.shape, u.dtype), u_near, lane)
    for step in range(1, lanes):
        u_all = put(u_all, shift(u_near, step), (lane - step) % lanes)
    u_all = u_all.reshape(lanes * u.shape[0], token_count)

    gram_tile = times(inner_t, panel, 1, 0) * (1.0 / token_count)

    grads_near = jnp.zeros((lanes,) + moved[0].shape, jnp.float32)
    for step in range(lanes):
        grads_near = put(grads_near, moved[step], (lane - step) % lanes)
    grads_near = grads_near.reshape(lanes * moved[0].shape[0], share)
    applied = times(inner_t, split(u_all * (1.0 / token_count), 0), 1, 1)
    columns = applied.shape[1] // 2
    applied = applied[:, :columns] + applied[:, columns:] + damping * grads_near.T
    return (gram_tile, applied, solution_t.T)


def solution(mesh):
    in_specs = (P("row", "col"), P("col", "row"))
    out_specs = (P("row", "col"), P("row", "col"), P("col", "row"))
    return jax.shard_map(step, mesh=mesh, in_specs=in_specs, out_specs=out_specs, check_vma=False)
```

```python
import math

import jax
import jax.numpy as jnp
from jax import lax
from jax.sharding import PartitionSpec as P


damping = 1.0


def step_size(feature_count, token_count):
    return 1.0 / (damping + (1.0 + math.sqrt(feature_count / token_count)) ** 2)


def split(value, axis):
    high = lax.reduce_precision(value, 8, 7)
    low = value - high
    return jnp.concatenate([high.astype(jnp.bfloat16), low.astype(jnp.bfloat16)], axis)


def merge(value):
    half = value.shape[0] // 2
    return value[:half] + value[half:]


def times(left, right, left_dim, right_dim):
    return lax.dot_general(
        left, right, (((left_dim,), (right_dim,)), ((), ())), preferred_element_type=jnp.float32
    )


def middle(z):
    return z in (1, 2)


def plan_inner(layers):
    if layers != 4:
        return [
            {(k, z): (z, k ^ turn) for k in range(layers) for z in range(layers)}
            for turn in range(layers)
        ], []
    flat = [
        {
            (k, z): (k ^ mask, z)
            for k in range(4)
            for z in range(4)
            if middle(z) or k ^ mask in (z, z ^ 1)
        }
        for mask in (1, 2, 3)
    ]
    outer = [
        {
            (k, z): ((2 if z == 1 else 0) + (turn ^ k), 0 if z == 1 else 3)
            for k in range(4)
            for z in (1, 2)
            if turn ^ k in (0, 1)
        }
        for turn in range(4)
    ]
    return flat, outer


def step(acts, grads):
    layers = lax.axis_size("col")
    lanes = lax.axis_size("row") // layers
    row_index = lax.axis_index("row")
    layer = lax.axis_index("col")
    group = row_index // lanes
    lane = row_index % lanes
    tokens, width = acts.shape
    share = width // lanes
    group_tokens = tokens * lanes
    token_count = group_tokens * layers
    omega = step_size(width * layers, token_count)
    bits = [1 << b for b in range(layers.bit_length() - 1)]

    def send(value, rule):
        pairs = []
        for k in range(layers):
            for j in range(lanes):
                for z in range(layers):
                    target = rule(k, j, z)
                    if target is not None:
                        to_k, to_j, to_z = target
                        pairs.append(
                            ((k * lanes + j) * layers + z, (to_k * lanes + to_j) * layers + to_z)
                        )
        return lax.ppermute(value, ("row", "col"), pairs)

    def shift(value, step):
        return send(value, lambda k, j, z: (k, (j + step) % lanes, z))

    def follow(value, plan):
        def rule(k, j, z):
            if (k, z) not in plan:
                return None
            to_k, to_z = plan[k, z]
            return (to_k, j, to_z)

        return send(value, rule)

    def put(whole, part, *spot):
        spot = spot + (0,) * (whole.ndim - len(spot))
        return lax.dynamic_update_slice(whole, part[(None,) * (whole.ndim - part.ndim)], spot)

    grads_t = grads.T

    panel = jnp.broadcast_to(acts, (layers, lanes, tokens, width))
    pieces = {0: acts}
    for mask in range(1, layers):
        pieces[mask] = send(acts, lambda k, j, z: (k ^ mask, j, z))
    swapped = [acts]
    for mask, piece in pieces.items():
        panel = put(panel, piece, group ^ mask, lane)
        for step in range(1, lanes):
            other = shift(piece, step)
            if mask == 0:
                swapped.append(other)
            panel = put(panel, other, group ^ mask, (lane - step) % lanes)
    panel = panel.reshape(token_count, width)

    mine = jnp.broadcast_to(
        lax.dynamic_slice_in_dim(acts, lane * share, share, 1), (lanes, tokens, share)
    )
    for step in range(1, lanes):
        cut = lax.dynamic_slice_in_dim(swapped[step], lane * share, share, 1)
        mine = put(mine, cut, (lane - step) % lanes)
    mine = put(mine, lax.dynamic_slice_in_dim(acts, lane * share, share, 1), lane)
    mine_t = mine.reshape(group_tokens, share).T

    flat, outer = plan_inner(layers)
    if layers == 4:
        held = jnp.broadcast_to(mine_t, (layers, share, group_tokens))
        ways = [
            ({0: 2, 3: 1}, (layer + 2) % 4),
            ({1: 2, 2: 1}, 3 - layer),
            ({0: 1, 1: 0, 2: 3, 3: 2}, layer ^ 1),
        ]
        for goes, spot in ways:
            part = send(mine_t, lambda k, j, z: (k, j, goes[z]) if z in goes else None)
            held = put(held, part, spot)
        held = put(held, mine_t, layer)

        def pick(index):
            return lax.dynamic_index_in_dim(held, index, 0, keepdims=False)

        inner_t = jnp.broadcast_to(pick(group), held.shape)
        for mask, plan in enumerate(flat, 1):
            inner_t = put(inner_t, follow(pick(group ^ mask), plan), group ^ mask)
        first = jnp.where(layer == 1, 2, 0)
        turned = [
            follow(pick(first + ((turn ^ group) & 1)), plan)
            for turn, plan in enumerate(outer)
        ]
        is_outer = ((layer == 0) & (group >= 2)) | ((layer == 3) & (group < 2))
        odd = group % 2 == 1
        inner_t = jnp.concatenate(
            [
                jnp.where(is_outer, jnp.where(odd, turned[p ^ 1], turned[p]), inner_t[p])
                for p in range(4)
            ],
            1,
        )
    else:
        inner_t = jnp.broadcast_to(mine_t, (layers, share, group_tokens))
        for turn, plan in enumerate(flat):
            inner_t = put(inner_t, follow(mine_t, plan), layer ^ turn)
        inner_t = inner_t.transpose(1, 0, 2).reshape(share, token_count)

    def by_lane(parts):
        rows = []
        for j in range(lanes):
            row = parts[0]
            for step in range(1, lanes):
                row = jnp.where((lane - step) % lanes == j, parts[step], row)
            rows.append(row)
        return jnp.concatenate(rows, 0)

    def layer_sum(value):
        for bit in bits:
            value = value + send(value, lambda k, j, z: (k, j, z ^ bit))
        return value

    def to_tokens(value):
        return merge(times(value, panel, 1, 1))

    def to_features(value):
        return merge(times(split(value * (1.0 / token_count), 0), panel, 1, 0))

    grads_split = split(grads_t, 0)
    u = to_tokens(grads_split)
    u = layer_sum(u)
    y = to_features(u) + damping * grads_t
    w = layer_sum(to_tokens(split(y, 0)))
    second = to_features(w) + damping * y
    solution_t = 3.0 * omega * grads_t - 3.0 * omega**2 * y + omega**3 * second

    moved = []
    for step in range(lanes):
        part = lax.dynamic_slice_in_dim(y, (lane + step) % lanes * share, share, 1)
        if step == 0:
            moved.append(send(part, lambda k, j, z: (z, j, k)))
        else:
            flips = [layers // 2 >> j % 2 for j in range(lanes)]
            part = send(part, lambda k, j, z: (k ^ flips[j], (j + step) % lanes, z))
            moved.append(send(part, lambda k, j, z: (z, j, k ^ flips[(j - step) % lanes])))
    applied = by_lane(moved).T

    gram_tile = times(inner_t, panel, 1, 0) * (1.0 / token_count)

    return (gram_tile, applied, solution_t.T)


def solution(mesh):
    in_specs = (P("row", "col"), P("col", "row"))
    out_specs = (P("row", "col"), P("row", "col"), P("col", "row"))
    return jax.shard_map(step, mesh=mesh, in_specs=in_specs, out_specs=out_specs, check_vma=False)
```
